64 devices in a mesh: dp: 4 (over x, y), dcp: 16 (over z, core).
Axes of the slice: x: 2, y: 2, z: 8, core: 2. Of those that a mesh axis runs over, the one named last changes fastest.
The devices are a block of a 4x4x8 slice.
Arguments:
- q: bfloat16 [64, 128, 576], P('dp', 'dcp'), parts along dimension 0
- cache: bfloat16 [64, 128, 16, 8, 576], P('dp', None, 'dcp'), parts along dimension 0
- lens: int32 [64], P('dp'), parts along dimension 0
Outputs:
- output: bfloat16 [64, 128, 512], P('dp', 'dcp'), parts along dimension 0
There are 4 independent parts. The reference program is written for one: setup_inputs(seed, part) draws one part's arguments, and reference() takes and returns one part's arrays. A program takes and returns all parts, laid end to end along the dimension named above; each array names one.
All inputs are finite; a program needn't handle non-finite values.
Results may differ from the reference program's by a relative error of at most 0.00646929.
Values are sent between devices in bfloat16 or wider.
A program may use at most 768 MiB of HBM per device.

```python
import jax
import jax.numpy as jnp
from jax import lax

B = 16
S = 16384
PAGE = 8
DCP = 16
HEADS = 128
LORA = 512
ROPE = 64
NOPE = 128

R = S // (PAGE * DCP)
K = LORA + ROPE


def setup_inputs(seed: int = 0, part: int = 0) -> dict:
    key = jax.random.fold_in(jax.random.key(seed), part)
    kq, kc, kl = jax.random.split(key, 3)
    qs = 1.5 * ((NOPE + ROPE) / 2.0) ** 0.5
    scale = jnp.concatenate([jnp.full((LORA,), qs / LORA ** 0.5, jnp.float32), jnp.full((ROPE,), qs / ROPE ** 0.5, jnp.float32)])
    q = (jax.random.normal(kq, (B, HEADS, K), jnp.float32) * scale).astype(jnp.bfloat16)
    cache = jax.random.normal(kc, (B, R, DCP, PAGE, K), jnp.float32).astype(jnp.bfloat16)
    lens = jax.random.randint(kl, (B,), S // 4, S + 1, jnp.int32)
    return {'q': q, 'cache': cache, 'lens': lens}


def reference(q, cache, lens):
    c = cache.reshape(B, S, K)
    pos = jnp.arange(S)

    def one(args):
        qb, cb, lb = args
        s = jnp.dot(qb, cb.T, preferred_element_type=jnp.float32) / (NOPE + ROPE) ** 0.5
        s = jnp.where(pos[None, :] < lb, s, -jnp.inf)
        a = jax.nn.softmax(s, axis=1)
        o = jnp.dot(a, cb[:, :LORA].astype(jnp.float32), preferred_element_type=jnp.float32)
        return o.astype(jnp.bfloat16)

    return lax.map(one, (q, c, lens))
```

```python
import functools
import jax
import jax.numpy as jnp
from jax import lax
from jax.experimental import pallas as pl
from jax.experimental.pallas import tpu as pltpu
from jax.sharding import PartitionSpec as P

ROPE = 64
QK_DIM = 192
SCALE = QK_DIM ** -0.5
NEG = -2.0e38
NB = 2
QB = 4
L2, L3, L4, L5 = 1, 3, 4, 5
MESH = pl.DeviceIdType.MESH
F32 = jnp.float32
BF16 = jnp.bfloat16


def mix(rows):
    top = functools.reduce(jnp.maximum, rows)
    ws = [jnp.exp(x - top) for x in rows]
    tot = functools.reduce(jnp.add, ws)
    inv = 1.0 / tot
    return [w * inv for w in ws], top + jnp.log(tot)


def kernel(n, page, lens_ref, q_ref, c_ref, o_ref,
           qg, cb, of, od, lf, ld, pw, pr, asnd, arcv, alsnd, alrcv, bsnd, brcv, blsnd, blrcv,
           r2s, r2r, r2ls, r2lr, r1s, r1r, r1ls, r1lr,
           csem, qsem, qss, qsr, qds, qdr, ods, odr, lds, ldr,
           ass, asr, alss, alsr, bss, bsr, blss, blsr,
           r2ss, r2sr, r2lss, r2lsr, r1ss, r1sr, r1lss, r1lsr):
    me = lax.axis_index('dcp')
    Z = n // 2
    H = Z // 2
    z = me // 2
    core = me % 2
    other = 1 - core
    peer = 2 * z + other
    nseq, hl, kd = q_ref.shape
    R = c_ref.shape[3]
    T = page * R
    lora = o_ref.shape[2]
    CH = nseq // NB
    CQ = nseq // QB
    DIRS = (1, -1)

    def chip(d):
        return (z + (d + Z)) % Z

    def dev(d):
        return 2 * chip(d) + core

    def remote(src, dst, ss, rs, to):
        return pltpu.make_async_remote_copy(src_ref=src, dst_ref=dst, send_sem=ss, recv_sem=rs,
                                            device_id={'dcp': to}, device_id_type=MESH)

    def mine(dv, lo, cnt):
        return qg.at[pl.ds(lo, cnt), pl.ds(pl.multiple_of(dv * hl, hl), hl), :]

    qcp = pltpu.make_async_copy(q_ref, mine(me, 0, nseq), qsem.at[0])
    qcp.start()

    bar = pltpu.get_barrier_semaphore()
    partners = [peer, dev(1), dev(-1), dev(2), dev(-2)]
    for t in partners:
        pl.semaphore_signal(bar, inc=1, device_id={'dcp': t}, device_id_type=MESH)

    def ccopy(i):
        return pltpu.make_async_copy(c_ref.at[i], cb.at[i], csem.at[i])

    qcp.wait()
    pl.semaphore_wait(bar, len(partners))

    def qring(si, h, c):
        s = DIRS[si]
        blk = mine(dev(-s * h), c * QB, QB)
        return remote(blk, blk, qss.at[si, h, c], qsr.at[si, h, c], dev(s))

    def qd2d(si, h, c):
        s = DIRS[si]
        blk = mine(dev(-s * (h + 1)), c * QB, QB)
        return remote(blk, blk, qds.at[si, h, c], qdr.at[si, h, c], peer)

    def qarrive(si, h, c):
        s = DIRS[si]
        blk = mine(2 * chip(-s * (h + 1)) + other, c * QB, QB)
        return remote(blk, blk, qds.at[si, h, c], qdr.at[si, h, c], peer)

    def qrecv(si, h, c):
        s = DIRS[si]
        blk = mine(dev(-s * (h + 1)), c * QB, QB)
        return remote(blk, blk, qss.at[si, h, c], qsr.at[si, h, c], dev(s))

    def half(si):
        return range(CQ // 2) if si == 0 else range(CQ // 2, CQ)

    sends = []
    own = mine(me, 0, nseq)
    for c in range(CQ):
        for si in range(2):
            x = qring(si, 0, c)
            x.start()
            sends.append(x)
    dself = remote(own, own, qsem.at[1], qsem.at[2], peer)
    dself.start()
    sends.append(dself)

    for i in range(nseq):
        ccopy(i).start()

    for h in range(H):
        for c in range(CQ):
            for si in range(2):
                if h == H - 1 and c not in half(si):
                    continue
                qrecv(si, h, c).wait_recv()
                if h < H - 2 or (h == H - 2 and c in half(si)):
                    x = qring(si, h + 1, c)
                    x.start()
                    sends.append(x)
                x = qd2d(si, h, c)
                x.start()
                sends.append(x)
    pown = mine(peer, 0, nseq)
    remote(pown, pown, qsem.at[1], qsem.at[2], peer).wait_recv()
    for h in range(H):
        for c in range(CQ):
            for si in range(2):
                if h == H - 1 and c not in half(si):
                    continue
                qarrive(si, h, c).wait_recv()

    lane = lax.broadcasted_iota(jnp.int32, (hl, 128), 1)
    sub = lax.broadcasted_iota(jnp.int32, (hl, 128), 0)
    row1 = lax.broadcasted_iota(jnp.int32, (1, 128), 1)
    tt = lax.broadcasted_iota(jnp.int32, (1, T), 1)
    pos = ((tt % R) * n + me) * page + tt // R

    def col(row, j):
        return jnp.sum(jnp.where(lane == j * hl + sub, row, 0.0), axis=1, keepdims=True)

    def d2d_o(k):
        return (remote(of.at[k, :, :, other], od.at[k], ods.at[k], odr.at[k], peer),
                remote(lf.at[k, :, other], ld.at[k], lds.at[k], ldr.at[k], peer))

    def compute(k):
        lses = []
        for j in range(NB):
            b = k * NB + j
            ccopy(b).wait()
            qb = qg[b]
            cc = jnp.concatenate([cb[b, i] for i in range(page)], axis=1)
            s = jnp.dot(qb, cc, preferred_element_type=F32) * SCALE
            s = jnp.where(pos < lens_ref[b], s, NEG)
            m = jnp.max(s, axis=1, keepdims=True)
            m = jnp.where(m > NEG, m, 0.0)
            p = jnp.exp(s - m)
            l = jnp.sum(p, axis=1, keepdims=True)
            has = l > 0.0
            ls = jnp.where(has, l, 1.0)
            vv = jnp.concatenate([cb[b, i, :lora] for i in range(page)], axis=1)
            acc = lax.dot_general(p.astype(BF16), vv, (((1,), (1,)), ((), ())), preferred_element_type=F32)
            acc = acc * (1.0 / ls)
            of[k, j] = acc.reshape(Z, 2, hl, lora)
            lses.append(jnp.where(has, m + jnp.log(ls), NEG))
        x = jnp.zeros((n * hl, 128), F32)
        lane2 = lax.broadcasted_iota(jnp.int32, (n * hl, 128), 1)
        row2 = lax.broadcasted_iota(jnp.int32, (n * hl, 128), 0) % hl
        for j in range(NB):
            x = jnp.where(lane2 == j * hl + row2, lses[j], x)
        x = jnp.sum(x.reshape(n, hl, 128), axis=1, keepdims=True)
        lf[k] = x.reshape(Z, 2, 1, 128)
        for x in d2d_o(k):
            x.start()

    def snd_a(si, k):
        to = dev(2 * DIRS[si])
        return (remote(asnd.at[si, k], arcv.at[si, k], ass.at[si, k], asr.at[si, k], to),
                remote(alsnd.at[si, k], alrcv.at[si, k], alss.at[si, k], alsr.at[si, k], to))

    def snd_b(si, k):
        to = dev(DIRS[si])
        return (remote(bsnd.at[si, k], brcv.at[si, k], bss.at[si, k], bsr.at[si, k], to),
                remote(blsnd.at[si, k], blrcv.at[si, k], blss.at[si, k], blsr.at[si, k], to))

    def snd_2(si, k):
        to = dev(DIRS[si])
        return (remote(r2s.at[si, k], r2r.at[si, k], r2ss.at[si, k], r2sr.at[si, k], to),
                remote(r2ls.at[si, k], r2lr.at[si, k], r2lss.at[si, k], r2lsr.at[si, k], to))

    def snd_1(si, k):
        to = dev(DIRS[si])
        return (remote(r1s.at[si, k], r1r.at[si, k], r1ss.at[si, k], r1sr.at[si, k], to),
                remote(r1ls.at[si, k], r1lr.at[si, k], r1lss.at[si, k], r1lsr.at[si, k], to))

    def stage2(k):
        for x in d2d_o(k):
            x.wait_recv()
        for d in (H, 3, -3, 2, -2, 1, -1, 0):
            t = chip(d)
            (a0, a1), lr = mix([lf[k, t, core], ld[k, t]])
            if d == H:
                for si in range(2):
                    alsnd[si, k] = jnp.where(row1 // hl == si, lr, NEG)
            elif abs(d) == 3:
                blsnd[0 if d > 0 else 1, k] = lr
            else:
                pr[d + 2, k] = lr
            for j in range(NB):
                o = col(a0, j) * of[k, j, t, core] + col(a1, j) * od[k, j, t]
                if d == H:
                    asnd[j, k] = o.astype(BF16)
                elif abs(d) == 3:
                    bsnd[0 if d > 0 else 1, k, j] = o.astype(BF16)
                else:
                    pw[d + 2, k, j] = o
        for si in range(2):
            for x in snd_a(si, k) + snd_b(si, k):
                x.start()

    def stage3(k):
        for si in range(2):
            for x in snd_a(si, k) + snd_b(si, k):
                x.wait_recv()
            d = 2 * DIRS[si]
            (a0, a1, a2), lr = mix([pr[d + 2, k], blrcv[si, k], alrcv[si, k]])
            for j in range(NB):
                o = col(a0, j) * pw[d + 2, k, j] + col(a1, j) * brcv[si, k, j].astype(F32)
                if j == si:
                    o = o + col(a2, j) * arcv[si, k].astype(F32)
                r2s[si, k, j] = o
            r2ls[si, k] = lr
            for x in snd_2(si, k):
                x.start()

    def stage4(k):
        for si in range(2):
            for x in snd_2(si, k):
                x.wait_recv()
            d = DIRS[si]
            (a0, a1), lr = mix([pr[d + 2, k], r2lr[si, k]])
            for j in range(NB):
                r1s[si, k, j] = col(a0, j) * pw[d + 2, k, j] + col(a1, j) * r2r[si, k, j]
            r1ls[si, k] = lr
            for x in snd_1(si, k):
                x.start()

    def stage5(k):
        for si in range(2):
            for x in snd_1(si, k):
                x.wait_recv()
        (a0, a1, a2), _ = mix([pr[2, k], r1lr[0, k], r1lr[1, k]])
        for j in range(NB):
            o = col(a0, j) * pw[2, k, j] + col(a1, j) * r1r[0, k, j] + col(a2, j) * r1r[1, k, j]
            o_ref[k * NB + j] = o.astype(BF16)

    def step(k, carry):
        @pl.when(k < CH)
        def _():
            compute(k)
        for lag, stage in ((L2, stage2), (L3, stage3), (L4, stage4), (L5, stage5)):
            @pl.when((k >= lag) & (k < CH + lag))
            def _(lag=lag, stage=stage):
                stage(k - lag)
        return carry

    lax.fori_loop(0, CH + L5, step, 0)

    for x in sends:
        x.wait_send()

    def drain(k, carry):
        for x in d2d_o(k):
            x.wait_send()
        for si in range(2):
            for x in snd_a(si, k) + snd_b(si, k) + snd_2(si, k) + snd_1(si, k):
                x.wait_send()
        return carry

    lax.fori_loop(0, CH, drain, 0)


def solution(mesh):
    n = mesh.shape['dcp']

    def local(q, cache, lens):
        b, hl, k = q.shape
        r = cache.shape[1]
        page = cache.shape[3]
        lora = k - ROPE
        T = r * page
        c = cache.reshape(b, r, page, k).transpose(0, 2, 3, 1)
        Z = n // 2
        CH = b // NB
        CQ = b // QB
        V = pltpu.VMEM
        D = pltpu.SemaphoreType.DMA
        scratch = [
            V((b, n * hl, k), BF16), V((b, page, k, r), BF16),
            V((CH, NB, Z, 2, hl, lora), F32), V((CH, NB, Z, hl, lora), F32),
            V((CH, Z, 2, 1, 128), F32), V((CH, Z, 1, 128), F32),
            V((5, CH, NB, hl, lora), F32), V((5, CH, 1, 128), F32),
            V((2, CH, hl, lora), BF16), V((2, CH, hl, lora), BF16), V((2, CH, 1, 128), F32), V((2, CH, 1, 128), F32),
            V((2, CH, NB, hl, lora), BF16), V((2, CH, NB, hl, lora), BF16), V((2, CH, 1, 128), F32), V((2, CH, 1, 128), F32),
            V((2, CH, NB, hl, lora), F32), V((2, CH, NB, hl, lora), F32), V((2, CH, 1, 128), F32), V((2, CH, 1, 128), F32),
            V((2, CH, NB, hl, lora), F32), V((2, CH, NB, hl, lora), F32), V((2, CH, 1, 128), F32), V((2, CH, 1, 128), F32),
            D((b,)), D((3,)),
            D((2, Z // 2, CQ)), D((2, Z // 2, CQ)), D((2, Z // 2, CQ)), D((2, Z // 2, CQ)),
            D((CH,)), D((CH,)), D((CH,)), D((CH,)),
        ] + [D((2, CH))] * 16
        return pl.pallas_call(
            functools.partial(kernel, n, page),
            out_shape=jax.ShapeDtypeStruct((b, hl, lora), BF16),
            in_specs=[pl.BlockSpec(memory_space=pltpu.SMEM), pl.BlockSpec(memory_space=pl.ANY),
                      pl.BlockSpec(memory_space=pl.ANY)],
            out_specs=pl.BlockSpec(memory_space=pltpu.VMEM),
            scratch_shapes=scratch,
            compiler_params=pltpu.CompilerParams(collective_id=0, has_side_effects=True,
                                                 vmem_limit_bytes=60 * 1024 * 1024),
        )(lens, q, c)

    return jax.shard_map(local, mesh=mesh, in_specs=(P('dp', 'dcp', None), P('dp', None, 'dcp', None, None), P('dp')), out_specs=P('dp', 'dcp', None), check_vma=False)
```
